32 devices in a mesh: dp: 4 (over x, core), tensor: 8 (over z, y).
Axes of the slice: x: 2, y: 2, z: 4, core: 2. Of those that a mesh axis runs over, the one named last changes fastest.
Arguments:
- head_outputs: bfloat16 [4096, 4096], P('dp', 'tensor'), may hold values from -6 to 6
- out_weight: bfloat16 [4096, 4096], P('tensor'), may hold values from -0.09375 to 0.09375
- residual: bfloat16 [4096, 4096], P(('dp', 'tensor')), may hold values from -6 to 6
- norm_gain: float32 [4096], replicated, may hold values from 0.25 to 1.75
- chosen: int32 [16, 256], replicated, may hold values from 0 to 4095, as said below
- gates: float32 [16, 256], replicated, may hold values from 0.25 to 1
- place: int32 [16], replicated, may hold values from 0 to 15, each once
- w_gate: bfloat16 [32, 704, 4096], P(('dp', 'tensor')), may hold values from -0.09375 to 0.09375
- w_up: bfloat16 [32, 704, 4096], P(('dp', 'tensor')), may hold values from -0.09375 to 0.09375
- w_down: bfloat16 [32, 704, 4096], P(('dp', 'tensor')), may hold values from -0.15625 to 0.15625
Outputs:
- mixed: bfloat16 [4096, 4096], P(('dp', 'tensor'))
The draws below stay inside these ranges and needn't reach their ends.
Inputs may be any that keep to these rules, and one draw needn't show every extreme that they name: `chosen`: row e lists 256 different tokens; at most 16 of them lie in one aligned block of 128 rows (the rows of one device), and in every row some block holds exactly 16.
All inputs are finite; a program needn't handle non-finite values.
Results may differ from the reference program's by a relative error of at most 0.012.
Values may be sent and summed in bfloat16 or wider, within the bound.
A program may use at most 128 MiB of HBM per device.

```python
import jax
import jax.numpy as jnp
from jax import lax

D = 4096
HEADS = 32
HEAD_DIM = 128
FF = 1408
TOK_DEV = 128
OWNERS = 32
EXPERTS = 16
TOKENS = 4096
CAP = 256
MOST = 16
N_TENSOR = 8


def draw_chosen(key, part):
    keys = jax.random.split(key, 4)
    popularity = jax.random.randint(keys[0], (OWNERS,), 0, 3)
    noise = jax.random.randint(keys[1], (EXPERTS, OWNERS), 0, 64)
    device_ids = jnp.arange(OWNERS, dtype=jnp.int32)
    ranking = (noise + 32 * popularity[None, :]) * OWNERS + device_ids[None, :]
    _, order = lax.top_k(ranking, OWNERS)
    position = jnp.argsort(order, axis=1)
    quarter = OWNERS // 4
    counts = jnp.where(position < quarter, MOST, jnp.where(position < 3 * quarter, MOST // 2, 0))
    shuffle = jax.random.randint(keys[2], (EXPERTS, OWNERS, TOK_DEV), 0, 4096) * TOK_DEV + jnp.arange(TOK_DEV, dtype=jnp.int32)[None, None, :]
    picks = jnp.argsort(shuffle, axis=2)[:, :, :MOST].astype(jnp.int32)
    candidates = device_ids[None, :, None] * TOK_DEV + picks
    live = (jnp.arange(MOST, dtype=jnp.int32)[None, None, :] < counts[:, :, None]).astype(jnp.int32)
    spread = OWNERS * MOST
    order_key = jax.random.randint(keys[3], (EXPERTS, spread), 0, 4096) * spread + jnp.arange(spread, dtype=jnp.int32)[None, :]
    priority = live.reshape(EXPERTS, spread) * (4096 * spread) + order_key
    _, slots = lax.top_k(priority, CAP)
    return jnp.take_along_axis(candidates.reshape(EXPERTS, spread), slots, axis=1).astype(jnp.int32)


def levels(rng, shape, cuts, smallest, largest):
    def one(axis_at, parts):
        draws = jax.random.uniform(jax.random.fold_in(jax.random.fold_in(rng, 6), axis_at), (parts,), jnp.float32, smallest / len(cuts), largest / len(cuts))
        return jnp.repeat(jnp.exp(draws), shape[axis_at] // parts).reshape((-1,) + (1,) * (len(shape) - axis_at - 1))

    factor_of = one(*cuts[0])
    for cut in cuts[1:]:
        factor_of = factor_of * one(*cut)
    return factor_of


def bell_draw(own_key, shape, scale, bound, pieces=(), kind=jnp.bfloat16):
    array = scale * jax.random.normal(own_key, shape, jnp.float32)
    if pieces:
        array = array * levels(own_key, shape, pieces, -0.22, 0.18)
    return jnp.clip(array, -bound, bound).astype(kind)


def setup_inputs(seed: int = 0) -> dict:
    streams_of = jax.random.split(jax.random.key(seed), 11)
    return {
        "head_outputs": bell_draw(streams_of[0], (TOKENS, HEADS * HEAD_DIM), 1.0, 6.0, ((0, 4), (1, 8))),
        "out_weight": bell_draw(streams_of[1], (HEADS * HEAD_DIM, D), (HEADS * HEAD_DIM) ** -0.5, 0.09375, ((0, 8),)),
        "residual": bell_draw(streams_of[2], (TOKENS, D), 1.0, 6.0, ((0, 32),)),
        "norm_gain": jnp.clip(1.0 + 0.15 * jax.random.normal(streams_of[3], (D,), jnp.float32), 0.25, 1.75),
        "chosen": draw_chosen(jax.random.fold_in(streams_of[10], 71), 0),
        "gates": jnp.clip(jax.random.uniform(streams_of[5], (EXPERTS, CAP), jnp.float32, 0.25, 1.0), 0.25, 1.0),
        "place": jax.random.permutation(streams_of[6], EXPERTS).astype(jnp.int32),
        "w_gate": bell_draw(streams_of[7], (OWNERS, FF // 2, D), D ** -0.5, 0.09375, ((0, 32),)),
        "w_up": bell_draw(streams_of[8], (OWNERS, FF // 2, D), D ** -0.5, 0.09375, ((0, 32),)),
        "w_down": bell_draw(streams_of[9], (OWNERS, FF // 2, D), FF ** -0.5, 0.15625, ((0, 32),)),
    }


def rounded(value):
    return lax.optimization_barrier(value.astype(jnp.bfloat16)).astype(jnp.float32)

def reference(head_outputs, out_weight, residual, norm_gain, chosen, gates, place, w_gate, w_up, w_down):
    block_cols = head_outputs.shape[1] // N_TENSOR
    projected = jnp.zeros((head_outputs.shape[0], out_weight.shape[1]), jnp.float32)
    for block in range(N_TENSOR):
        left = head_outputs[:, block * block_cols:(block + 1) * block_cols]
        right = out_weight[block * block_cols:(block + 1) * block_cols]
        projected = projected + rounded(jnp.dot(left, right, preferred_element_type=jnp.float32))
    layer_state = residual.astype(jnp.float32) + projected
    scale = lax.rsqrt(lax.optimization_barrier(jnp.mean(layer_state * layer_state, axis=1, keepdims=True)) + 1.0)
    normed = (layer_state * scale * norm_gain.astype(jnp.float32)[None, :]).astype(jnp.bfloat16)
    contract = (((1,), (1,)), ((), ()))

    def expert_step(carry, inputs):
        token_rows, gate_row, slot = inputs
        inputs_rows = normed[token_rows]
        summed = jnp.zeros((token_rows.shape[0], normed.shape[1]), jnp.float32)
        for half in range(2):
            index = (2 * slot + half).astype(jnp.int32)
            gate_half = lax.dynamic_index_in_dim(w_gate, index, 0, keepdims=False)
            up_half = lax.dynamic_index_in_dim(w_up, index, 0, keepdims=False)
            down_half = lax.dynamic_index_in_dim(w_down, index, 0, keepdims=False)
            gate_part = lax.dot_general(inputs_rows, gate_half, contract, preferred_element_type=jnp.float32)
            up_part = lax.dot_general(inputs_rows, up_half, contract, preferred_element_type=jnp.float32)
            hidden = (jax.nn.silu(gate_part) * up_part).astype(jnp.bfloat16)
            half_out = jnp.dot(hidden, down_half, preferred_element_type=jnp.float32).astype(jnp.bfloat16)
            summed = summed + half_out.astype(jnp.float32)
        return (carry.at[token_rows].add(gate_row.astype(jnp.float32)[:, None] * summed), None)
    moe, _ = lax.scan(expert_step, jnp.zeros(layer_state.shape, jnp.float32), (chosen, gates, place))
    return (layer_state + moe).astype(jnp.bfloat16)
```

```python
import functools

import jax
import jax.numpy as jnp
from jax import lax
from jax.experimental import pallas as pl
from jax.experimental.pallas import tpu as pltpu
from jax.sharding import PartitionSpec as P

MESH = pl.DeviceIdType.MESH
LANES = 4


def ring_rank(position, count):
    upper = position // (count // 2)
    return (1 - upper) * 2 * position + upper * (2 * (count - 1 - position) + 1)


def project_kernel(count, x_ref, w_ref, out_ref, held, term, send_sem, recv_sem):
    dp = lax.axis_index("dp")
    rank = lax.axis_index("tensor")
    odd = rank % 2
    half = rank // 2
    here = (1 - odd) * half + odd * (count - 1 - half)
    right = ring_rank((here + 1) % count, count)
    left = ring_rank((here + count - 1) % count, count)
    rows = out_ref.shape[0]
    width = out_ref.shape[1] // LANES

    def own_term(lane, block):
        start = pl.multiple_of(ring_rank(block, count) * rows, rows)
        return jnp.dot(
            x_ref[pl.ds(start, rows), :],
            w_ref[:, lane * width : (lane + 1) * width],
            preferred_element_type=jnp.float32,
        )

    def block_of(lane, slot):
        if lane < LANES // 2:
            return (here + 2 * count - 1 - slot) % count
        return (here + 1 + slot) % count

    def copy(lane, slot):
        return pltpu.make_async_remote_copy(
            src_ref=held.at[lane, slot],
            dst_ref=held.at[lane, slot + 1],
            send_sem=send_sem.at[lane, slot],
            recv_sem=recv_sem.at[lane, slot + 1],
            device_id=(dp, right if lane < LANES // 2 else left),
            device_id_type=MESH,
        )

    def arrival(lane, slot):
        return pltpu.make_async_remote_copy(
            src_ref=held.at[lane, slot],
            dst_ref=held.at[lane, slot],
            send_sem=send_sem.at[lane, slot],
            recv_sem=recv_sem.at[lane, slot],
            device_id=(dp, right if lane < LANES // 2 else left),
            device_id_type=MESH,
        )

    order = [lane for k in range(LANES // 2) for lane in (k, LANES // 2 + k)]
    barrier = pltpu.get_barrier_semaphore()
    for neighbour in (left, right):
        pl.semaphore_signal(barrier, inc=1, device_id=(dp, neighbour), device_id_type=MESH)
    for n, lane in enumerate(order):
        held[lane, 0] = own_term(lane, block_of(lane, 0)).astype(held.dtype)
        if n == 0:
            pl.semaphore_wait(barrier, 2)
        copy(lane, 0).start()

    def step(slot, carry):
        for lane in order:
            term[lane] = own_term(lane, block_of(lane, slot))
        for lane in order:
            arrival(lane, slot).wait_recv()
            held[lane, slot] = (held[lane, slot].astype(jnp.float32) + term[lane]).astype(held.dtype)
            copy(lane, slot).start()
        return carry

    lax.fori_loop(1, count - 1, step, 0)
    last = count - 1
    for lane in order:
        term[lane] = own_term(lane, block_of(lane, last))
    for lane in order:
        arrival(lane, last).wait_recv()
        out_ref[:, lane * width : (lane + 1) * width] = (
            held[lane, last].astype(jnp.float32) + term[lane]
        )

    def drain(slot, carry):
        for lane in order:
            copy(lane, slot).wait_send()
        return carry

    lax.fori_loop(0, count - 1, drain, 0)


def project(x, w, count):
    rows = x.shape[0] // count
    columns = w.shape[1]
    width = columns // LANES
    return pl.pallas_call(
        functools.partial(project_kernel, count),
        out_shape=jax.ShapeDtypeStruct((rows, columns), jnp.float32),
        in_specs=[pl.BlockSpec(memory_space=pltpu.VMEM)] * 2,
        out_specs=pl.BlockSpec(memory_space=pltpu.VMEM),
        scratch_shapes=[
            pltpu.VMEM((LANES, count, rows, width), jnp.bfloat16),
            pltpu.VMEM((LANES, rows, width), jnp.float32),
            pltpu.SemaphoreType.DMA((LANES, count)),
            pltpu.SemaphoreType.DMA((LANES, count)),
        ],
        compiler_params=pltpu.CompilerParams(
            collective_id=0, has_side_effects=True, vmem_limit_bytes=48 * 1024 * 1024
        ),
    )(x, w)


class Place:
    def __init__(self, replicas, count):
        self.dp = lax.axis_index("dp")
        rank = lax.axis_index("tensor")
        self.odd = rank % 2
        self.per_row = count // 2
        self.pairs = replicas * self.per_row
        self.pair = self.dp * self.per_row + rank // 2
        self.partner = (self.dp, rank + 1 - 2 * self.odd)

    def device(self, pair):
        return (pair // self.per_row, 2 * (pair % self.per_row) + self.odd)

    def greet(self):
        barrier = pltpu.get_barrier_semaphore()

        def signal(k, carry):
            target = self.device((self.pair + k) % self.pairs)
            pl.semaphore_signal(barrier, inc=1, device_id=target, device_id_type=MESH)
            return carry

        lax.fori_loop(1, self.pairs, signal, 0)
        pl.semaphore_signal(barrier, inc=1, device_id=self.partner, device_id_type=MESH)
        pl.semaphore_wait(barrier, self.pairs)


def loop(start, stop, body):
    def step(k, carry):
        body(k)
        return carry

    lax.fori_loop(start, stop, step, 0)


def dispatch_kernel(replicas, count, x_ref, out_ref, send_sem, pass_sem, recv_sem, local_sem):
    at = Place(replicas, count)
    me = 2 * at.pair + at.odd

    def outward(k):
        target = (at.pair + k) % at.pairs
        return pltpu.make_async_remote_copy(
            src_ref=x_ref.at[target],
            dst_ref=out_ref.at[me],
            send_sem=send_sem.at[k],
            recv_sem=recv_sem.at[me],
            device_id=at.device(target),
            device_id_type=MESH,
        )

    def across(k):
        slot = 2 * ((at.pair + at.pairs - k) % at.pairs) + at.odd
        return pltpu.make_async_remote_copy(
            src_ref=out_ref.at[slot],
            dst_ref=out_ref.at[slot],
            send_sem=pass_sem.at[k],
            recv_sem=recv_sem.at[slot],
            device_id=at.partner,
            device_id_type=MESH,
        )

    own = pltpu.make_async_remote_copy(
        src_ref=x_ref.at[at.pair],
        dst_ref=out_ref.at[me],
        send_sem=pass_sem.at[0],
        recv_sem=recv_sem.at[me],
        device_id=at.partner,
        device_id_type=MESH,
    )
    keep = pltpu.make_async_copy(x_ref.at[at.pair], out_ref.at[me], local_sem.at[0])
    at.greet()
    loop(1, at.pairs, lambda k: outward(k).start())
    own.start()
    keep.start()

    def forward(k):
        across(k).wait_recv()
        across(k).start()

    loop(1, at.pairs, forward)

    def settle(k):
        slot = 2 * ((at.pair + at.pairs - k) % at.pairs) + 1 - at.odd
        pltpu.make_async_remote_copy(
            src_ref=out_ref.at[slot],
            dst_ref=out_ref.at[slot],
            send_sem=pass_sem.at[k],
            recv_sem=recv_sem.at[slot],
            device_id=at.partner,
            device_id_type=MESH,
        ).wait_recv()

    loop(0, at.pairs, settle)
    keep.wait()
    own.wait_send()

    def drain(k):
        outward(k).wait_send()
        across(k).wait_send()

    loop(1, at.pairs, drain)


def dispatch(x, replicas, count):
    pairs = x.shape[0]
    return pl.pallas_call(
        functools.partial(dispatch_kernel, replicas, count),
        out_shape=jax.ShapeDtypeStruct((2 * pairs,) + x.shape[1:], x.dtype),
        in_specs=[pl.BlockSpec(memory_space=pltpu.VMEM)],
        out_specs=pl.BlockSpec(memory_space=pl.ANY),
        scratch_shapes=[
            pltpu.SemaphoreType.DMA((pairs,)),
            pltpu.SemaphoreType.DMA((pairs,)),
            pltpu.SemaphoreType.DMA((2 * pairs,)),
            pltpu.SemaphoreType.DMA((1,)),
        ],
        compiler_params=pltpu.CompilerParams(
            collective_id=1, has_side_effects=True, vmem_limit_bytes=48 * 1024 * 1024
        ),
    )(x)


def give_back_kernel(
    replicas, count, y_ref, out_ref, part, pass_sem, part_sem, send_sem, recv_sem, local_sem
):
    at = Place(replicas, count)

    def across(k):
        target = (at.pair + k) % at.pairs
        return pltpu.make_async_remote_copy(
            src_ref=y_ref.at[2 * target + 1 - at.odd],
            dst_ref=part.at[target],
            send_sem=pass_sem.at[k],
            recv_sem=part_sem.at[target],
            device_id=at.partner,
            device_id_type=MESH,
        )

    def home(k):
        target = (at.pair + k) % at.pairs
        return pltpu.make_async_remote_copy(
            src_ref=part.at[target],
            dst_ref=out_ref.at[at.pair],
            send_sem=send_sem.at[k],
            recv_sem=recv_sem.at[at.pair],
            device_id=at.device(target),
            device_id_type=MESH,
        )

    def add(k):
        across(k).wait_recv()
        target = (at.pair + k) % at.pairs
        part[target] = (
            part[target].astype(jnp.float32) + y_ref[2 * target + at.odd].astype(jnp.float32)
        ).astype(part.dtype)

    at.greet()
    loop(1, at.pairs, lambda k: across(k).start())
    across(0).start()

    def step(k):
        add(k)
        home(k).start()

    loop(1, at.pairs, step)
    add(0)
    keep = pltpu.make_async_copy(part.at[at.pair], out_ref.at[at.pair], local_sem.at[0])
    keep.start()

    def settle(k):
        source = (at.pair + at.pairs - k) % at.pairs
        pltpu.make_async_remote_copy(
            src_ref=part.at[source],
            dst_ref=out_ref.at[source],
            send_sem=send_sem.at[k],
            recv_sem=recv_sem.at[source],
            device_id=at.partner,
            device_id_type=MESH,
        ).wait_recv()

    loop(1, at.pairs, settle)
    keep.wait()
    across(0).wait_send()

    def drain(k):
        across(k).wait_send()
        home(k).wait_send()

    loop(1, at.pairs, drain)


def give_back(y, replicas, count):
    pairs = y.shape[0] // 2
    return pl.pallas_call(
        functools.partial(give_back_kernel, replicas, count),
        out_shape=jax.ShapeDtypeStruct((pairs,) + y.shape[1:], y.dtype),
        in_specs=[pl.BlockSpec(memory_space=pltpu.VMEM)],
        out_specs=pl.BlockSpec(memory_space=pl.ANY),
        scratch_shapes=[
            pltpu.VMEM((pairs,) + y.shape[1:], y.dtype),
            pltpu.SemaphoreType.DMA((pairs,)),
            pltpu.SemaphoreType.DMA((pairs,)),
            pltpu.SemaphoreType.DMA((pairs,)),
            pltpu.SemaphoreType.DMA((pairs,)),
            pltpu.SemaphoreType.DMA((1,)),
        ],
        compiler_params=pltpu.CompilerParams(
            collective_id=2, has_side_effects=True, vmem_limit_bytes=48 * 1024 * 1024
        ),
    )(y)


def on_device(
    head_outputs, out_weight, residual, norm_gain, chosen, gates, place, w_gate, w_up, w_down
):
    tensor_count = lax.axis_size("tensor")
    replica_count = lax.axis_size("dp")
    owners = replica_count * tensor_count
    my_index = lax.axis_index("dp") * tensor_count + lax.axis_index("tensor")
    row_count = residual.shape[0]
    model_width = residual.shape[1]
    projected = project(head_outputs, out_weight, tensor_count)
    layer_state = residual.astype(jnp.float32) + projected
    scale = lax.rsqrt(jnp.mean(layer_state * layer_state, axis=1, keepdims=True) + 1.0)
    normed = (layer_state * scale * norm_gain[None, :]).astype(jnp.bfloat16)
    experts = place.shape[0]
    capacity = chosen.shape[1]
    most = 2 * capacity // owners
    pair_map = (place[None, :] == jnp.arange(experts, dtype=jnp.int32)[:, None]).astype(jnp.float32)
    chosen_pair = jnp.dot(
        pair_map, chosen.astype(jnp.float32), precision=lax.Precision.HIGHEST
    ).astype(jnp.int32)
    gates_pair = jnp.dot(pair_map, gates, precision=lax.Precision.HIGHEST)
    local_row = chosen_pair - my_index * row_count
    is_mine = (local_row >= 0) & (local_row < row_count)
    mine_float = is_mine.astype(jnp.float32)
    capacity_ids = jnp.arange(capacity, dtype=jnp.int32)
    earlier = (capacity_ids[:, None] < capacity_ids[None, :]).astype(jnp.float32)
    slot_rank = jnp.dot(mine_float, earlier, precision=lax.Precision.HIGHEST).astype(jnp.int32)
    matches = is_mine[:, :, None] & (
        slot_rank[:, :, None] == jnp.arange(most, dtype=jnp.int32)[None, None, :]
    )
    match_count = matches.astype(jnp.int32)
    send_row = jnp.sum(match_count * local_row[:, :, None], axis=1)
    send_valid = jnp.sum(match_count, axis=1) > 0
    send_gate = jnp.sum(jnp.where(matches, gates_pair[:, :, None], 0.0), axis=1)
    targets = send_row.reshape(-1)
    valid_flat = send_valid.reshape(-1)
    row_ids = jnp.arange(row_count, dtype=jnp.int32)
    selector = ((targets[:, None] == row_ids[None, :]) & valid_flat[:, None]).astype(jnp.bfloat16)
    picked = jnp.dot(selector, normed, preferred_element_type=jnp.float32).astype(jnp.bfloat16)
    picked = picked.reshape(experts, most, model_width)
    received = dispatch(picked, replica_count, tensor_count)
    layout = received.shape
    flat = received.reshape(-1, layout[-1])
    contract = (((1,), (1,)), ((), ()))
    gate_part = lax.dot_general(flat, w_gate[0], contract, preferred_element_type=jnp.float32)
    up_part = lax.dot_general(flat, w_up[0], contract, preferred_element_type=jnp.float32)
    hidden = (jax.nn.silu(gate_part) * up_part).astype(jnp.bfloat16)
    result = jnp.dot(hidden, w_down[0], preferred_element_type=jnp.float32).astype(jnp.bfloat16)
    returned = give_back(result.reshape(layout), replica_count, tensor_count)
    summed = returned.reshape(experts * most, model_width).astype(jnp.float32)
    combine = jnp.where(
        (targets[None, :] == row_ids[:, None]) & valid_flat[None, :],
        send_gate.reshape(-1)[None, :],
        0.0,
    )
    moe = jnp.dot(combine, summed, precision=lax.Precision.HIGHEST)
    return (layer_state + moe).astype(jnp.bfloat16)


def solution(mesh):
    return jax.shard_map(
        on_device,
        mesh=mesh,
        in_specs=(
            P("dp", "tensor"),
            P("tensor", None),
            P(("dp", "tensor"), None),
            P(),
            P(),
            P(),
            P(),
            P(("dp", "tensor"), None, None),
            P(("dp", "tensor"), None, None),
            P(("dp", "tensor"), None, None),
        ),
        out_specs=P(("dp", "tensor"), None),
        check_vma=False,
    )
```

```python
import functools

import jax
import jax.numpy as jnp
from jax import lax
from jax.experimental import pallas as pl
from jax.experimental.pallas import tpu as pltpu
from jax.sharding import PartitionSpec as P

MESH = pl.DeviceIdType.MESH
LANES = 4


def ring_rank(position, count):
    upper = position // (count // 2)
    return (1 - upper) * 2 * position + upper * (2 * (count - 1 - position) + 1)


def project_kernel(count, x_ref, w_ref, out_ref, held, term, send_sem, recv_sem):
    dp = lax.axis_index("dp")
    rank = lax.axis_index("tensor")
    odd = rank % 2
    half = rank // 2
    here = (1 - odd) * half + odd * (count - 1 - half)
    right = ring_rank((here + 1) % count, count)
    left = ring_rank((here + count - 1) % count, count)
    rows = out_ref.shape[0]
    width = out_ref.shape[1] // LANES

    def own_term(lane, block):
        start = pl.multiple_of(ring_rank(block, count) * rows, rows)
        return jnp.dot(
            x_ref[pl.ds(start, rows), :],
            w_ref[:, lane * width : (lane + 1) * width],
            preferred_element_type=jnp.float32,
        )

    def block_of(lane, slot):
        if lane < LANES // 2:
            return (here + 2 * count - 1 - slot) % count
        return (here + 1 + slot) % count

    def copy(lane, slot):
        return pltpu.make_async_remote_copy(
            src_ref=held.at[lane, slot],
            dst_ref=held.at[lane, slot + 1],
            send_sem=send_sem.at[lane, slot],
            recv_sem=recv_sem.at[lane, slot + 1],
            device_id=(dp, right if lane < LANES // 2 else left),
            device_id_type=MESH,
        )

    def arrival(lane, slot):
        return pltpu.make_async_remote_copy(
            src_ref=held.at[lane, slot],
            dst_ref=held.at[lane, slot],
            send_sem=send_sem.at[lane, slot],
            recv_sem=recv_sem.at[lane, slot],
            device_id=(dp, right if lane < LANES // 2 else left),
            device_id_type=MESH,
        )

    order = [lane for k in range(LANES // 2) for lane in (k, LANES // 2 + k)]
    barrier = pltpu.get_barrier_semaphore()
    for neighbour in (left, right):
        pl.semaphore_signal(barrier, inc=1, device_id=(dp, neighbour), device_id_type=MESH)
    for n, lane in enumerate(order):
        held[lane, 0] = own_term(lane, block_of(lane, 0)).astype(held.dtype)
        if n == 0:
            pl.semaphore_wait(barrier, 2)
        copy(lane, 0).start()

    def step(slot, carry):
        for lane in order:
            term[lane] = own_term(lane, block_of(lane, slot))
        for lane in order:
            arrival(lane, slot).wait_recv()
            held[lane, slot] = (held[lane, slot].astype(jnp.float32) + term[lane]).astype(held.dtype)
            copy(lane, slot).start()
        return carry

    lax.fori_loop(1, count - 1, step, 0)
    last = count - 1
    for lane in order:
        term[lane] = own_term(lane, block_of(lane, last))
    for lane in order:
        arrival(lane, last).wait_recv()
        out_ref[:, lane * width : (lane + 1) * width] = (
            held[lane, last].astype(jnp.float32) + term[lane]
        )

    def drain(slot, carry):
        for lane in order:
            copy(lane, slot).wait_send()
        return carry

    lax.fori_loop(0, count - 1, drain, 0)


def project(x, w, count):
    rows = x.shape[0] // count
    columns = w.shape[1]
    width = columns // LANES
    return pl.pallas_call(
        functools.partial(project_kernel, count),
        out_shape=jax.ShapeDtypeStruct((rows, columns), jnp.float32),
        in_specs=[pl.BlockSpec(memory_space=pltpu.VMEM)] * 2,
        out_specs=pl.BlockSpec(memory_space=pltpu.VMEM),
        scratch_shapes=[
            pltpu.VMEM((LANES, count, rows, width), jnp.bfloat16),
            pltpu.VMEM((LANES, rows, width), jnp.float32),
            pltpu.SemaphoreType.DMA((LANES, count)),
            pltpu.SemaphoreType.DMA((LANES, count)),
        ],
        compiler_params=pltpu.CompilerParams(
            collective_id=0, has_side_effects=True, vmem_limit_bytes=48 * 1024 * 1024
        ),
    )(x, w)


class Place:
    def __init__(self, replicas, count):
        self.dp = lax.axis_index("dp")
        rank = lax.axis_index("tensor")
        self.odd = rank % 2
        self.per_row = count // 2
        self.pairs = replicas * self.per_row
        self.pair = self.dp * self.per_row + rank // 2
        self.partner = (self.dp, rank + 1 - 2 * self.odd)

    def device(self, pair):
        return (pair // self.per_row, 2 * (pair % self.per_row) + self.odd)

    def greet(self):
        barrier = pltpu.get_barrier_semaphore()

        def signal(k, carry):
            target = self.device((self.pair + k) % self.pairs)
            pl.semaphore_signal(barrier, inc=1, device_id=target, device_id_type=MESH)
            return carry

        lax.fori_loop(1, self.pairs, signal, 0)
        pl.semaphore_signal(barrier, inc=1, device_id=self.partner, device_id_type=MESH)
        pl.semaphore_wait(barrier, self.pairs)


def loop(start, stop, body):
    def step(k, carry):
        body(k)
        return carry

    lax.fori_loop(start, stop, step, 0)


PIECES = 4


def experts_kernel(
    replicas,
    count,
    group,
    x_ref,
    gate_hbm,
    up_hbm,
    down_hbm,
    out_ref,
    gate_w,
    up_w,
    down_w,
    received,
    result,
    part,
    weight_sem,
    send_sem,
    pass_sem,
    recv_sem,
    cross_sem,
    part_sem,
    home_sem,
    done_sem,
    keep_sem,
):
    at = Place(replicas, count)
    most, width = x_ref.shape[1:]
    rows = group * 2 * most
    groups = at.pairs // group

    def source(k):
        return (at.pair + at.pairs - k) % at.pairs

    def outward(k):
        target = (at.pair + k) % at.pairs
        return pltpu.make_async_remote_copy(
            src_ref=x_ref.at[target],
            dst_ref=received.at[k, at.odd],
            send_sem=send_sem.at[k],
            recv_sem=recv_sem.at[k, at.odd],
            device_id=at.device(target),
            device_id_type=MESH,
        )

    def sideways(k, side):
        return pltpu.make_async_remote_copy(
            src_ref=received.at[k, side],
            dst_ref=received.at[k, side],
            send_sem=pass_sem.at[k],
            recv_sem=recv_sem.at[k, side],
            device_id=at.partner,
            device_id_type=MESH,
        )

    def across(k):
        return pltpu.make_async_remote_copy(
            src_ref=result.at[k, 1 - at.odd],
            dst_ref=part.at[k],
            send_sem=cross_sem.at[k],
            recv_sem=part_sem.at[k],
            device_id=at.partner,
            device_id_type=MESH,
        )

    def home(k):
        return pltpu.make_async_remote_copy(
            src_ref=part.at[k],
            dst_ref=out_ref.at[at.pair],
            send_sem=home_sem.at[k],
            recv_sem=done_sem.at[at.pair],
            device_id=at.device(source(k)),
            device_id_type=MESH,
        )

    def forward(k):
        sideways(k, at.odd).wait_recv()
        sideways(k, at.odd).start()

    def add(k):
        across(k).wait_recv()
        part[k] = (
            part[k].astype(jnp.float32) + result[k, at.odd].astype(jnp.float32)
        ).astype(part.dtype)

    def add_and_send(k):
        add(k)
        home(k).start()

    loads = [
        pltpu.make_async_copy(hbm.at[0], vmem, weight_sem.at[n])
        for n, (hbm, vmem) in enumerate(((gate_hbm, gate_w), (up_hbm, up_w), (down_hbm, down_w)))
    ]
    for load in loads:
        load.start()
    own = pltpu.make_async_remote_copy(
        src_ref=x_ref.at[at.pair],
        dst_ref=received.at[0, at.odd],
        send_sem=pass_sem.at[0],
        recv_sem=recv_sem.at[0, at.odd],
        device_id=at.partner,
        device_id_type=MESH,
    )
    at.greet()
    loop(1, at.pairs, lambda k: outward(k).start())
    own.start()
    received[0, at.odd] = x_ref[at.pair]
    loop(1, group, forward)
    for load in loads:
        load.wait()
    contract = (((1,), (1,)), ((), ()))

    def step(g):
        first = g * group

        def forward_piece(piece):
            @pl.when(g + 1 < groups)
            def _():
                start = first + group
                cut = [start + n * group // PIECES for n in (piece, piece + 1)]
                loop(cut[0], cut[1], forward)

        loop(first, first + group, lambda k: sideways(k, 1 - at.odd).wait_recv())
        x = received[pl.ds(first, group)].reshape(rows, width)
        gate_part = lax.dot_general(x, gate_w[...], contract, preferred_element_type=jnp.float32)
        forward_piece(0)
        up_part = lax.dot_general(x, up_w[...], contract, preferred_element_type=jnp.float32)
        hidden = (gate_part / (1.0 + jnp.exp(-gate_part)) * up_part).astype(result.dtype)

        @pl.when(g > 0)
        def _():
            loop(jnp.maximum(first - group, 1), first, add_and_send)

        forward_piece(1)
        for piece in range(2):
            columns = slice(piece * (width // 2), (piece + 1) * (width // 2))
            y = jnp.dot(hidden, down_w[:, columns], preferred_element_type=jnp.float32)
            result[pl.ds(first, group), :, :, columns] = y.astype(result.dtype).reshape(
                group, 2, most, width // 2
            )
            forward_piece(2 + piece)
        loop(first, first + group, lambda k: across(k).start())

    loop(0, groups, step)
    loop(at.pairs - group, at.pairs, add_and_send)
    add(0)
    keep = pltpu.make_async_copy(part.at[0], out_ref.at[at.pair], keep_sem.at[0])
    keep.start()

    def settle(k):
        pair = source(k)
        pltpu.make_async_remote_copy(
            src_ref=part.at[k],
            dst_ref=out_ref.at[pair],
            send_sem=home_sem.at[k],
            recv_sem=done_sem.at[pair],
            device_id=at.partner,
            device_id_type=MESH,
        ).wait_recv()

    loop(1, at.pairs, settle)
    keep.wait()
    own.wait_send()
    across(0).wait_send()

    def drain(k):
        outward(k).wait_send()
        sideways(k, at.odd).wait_send()
        across(k).wait_send()
        home(k).wait_send()

    loop(1, at.pairs, drain)


def experts_layer(x, w_gate, w_up, w_down, replicas, count):
    pairs, most, width = x.shape
    group = min(pairs // 2, max(PIECES, 64 // most))
    hidden_units = w_gate.shape[1]
    weight = pltpu.VMEM((hidden_units, width), w_gate.dtype)
    return pl.pallas_call(
        functools.partial(experts_kernel, replicas, count, group),
        out_shape=jax.ShapeDtypeStruct(x.shape, x.dtype),
        in_specs=[pl.BlockSpec(memory_space=pltpu.VMEM)] + [pl.BlockSpec(memory_space=pl.ANY)] * 3,
        out_specs=pl.BlockSpec(memory_space=pl.ANY),
        scratch_shapes=[
            weight,
            weight,
            weight,
            pltpu.VMEM((pairs, 2, most, width), x.dtype),
            pltpu.VMEM((pairs, 2, most, width), x.dtype),
            pltpu.VMEM((pairs, most, width), x.dtype),
            pltpu.SemaphoreType.DMA((3,)),
            pltpu.SemaphoreType.DMA((pairs,)),
            pltpu.SemaphoreType.DMA((pairs,)),
            pltpu.SemaphoreType.DMA((pairs, 2)),
            pltpu.SemaphoreType.DMA((pairs,)),
            pltpu.SemaphoreType.DMA((pairs,)),
            pltpu.SemaphoreType.DMA((pairs,)),
            pltpu.SemaphoreType.DMA((pairs,)),
            pltpu.SemaphoreType.DMA((1,)),
        ],
        compiler_params=pltpu.CompilerParams(
            collective_id=1, has_side_effects=True, vmem_limit_bytes=56 * 1024 * 1024
        ),
    )(x, w_gate, w_up, w_down)


def on_device(
    head_outputs, out_weight, residual, norm_gain, chosen, gates, place, w_gate, w_up, w_down
):
    tensor_count = lax.axis_size("tensor")
    replica_count = lax.axis_size("dp")
    owners = replica_count * tensor_count
    my_index = lax.axis_index("dp") * tensor_count + lax.axis_index("tensor")
    row_count = residual.shape[0]
    model_width = residual.shape[1]
    projected = project(head_outputs, out_weight, tensor_count)
    layer_state = residual.astype(jnp.float32) + projected
    scale = lax.rsqrt(jnp.mean(layer_state * layer_state, axis=1, keepdims=True) + 1.0)
    normed = (layer_state * scale * norm_gain[None, :]).astype(jnp.bfloat16)
    experts = place.shape[0]
    capacity = chosen.shape[1]
    most = 2 * capacity // owners
    pair_map = (place[None, :] == jnp.arange(experts, dtype=jnp.int32)[:, None]).astype(jnp.float32)
    chosen_pair = jnp.dot(
        pair_map, chosen.astype(jnp.float32), precision=lax.Precision.HIGHEST
    ).astype(jnp.int32)
    gates_pair = jnp.dot(pair_map, gates, precision=lax.Precision.HIGHEST)
    local_row = chosen_pair - my_index * row_count
    is_mine = (local_row >= 0) & (local_row < row_count)
    mine_float = is_mine.astype(jnp.float32)
    capacity_ids = jnp.arange(capacity, dtype=jnp.int32)
    earlier = (capacity_ids[:, None] < capacity_ids[None, :]).astype(jnp.float32)
    slot_rank = jnp.dot(mine_float, earlier, precision=lax.Precision.HIGHEST).astype(jnp.int32)
    matches = is_mine[:, :, None] & (
        slot_rank[:, :, None] == jnp.arange(most, dtype=jnp.int32)[None, None, :]
    )
    match_count = matches.astype(jnp.int32)
    send_row = jnp.sum(match_count * local_row[:, :, None], axis=1)
    send_valid = jnp.sum(match_count, axis=1) > 0
    send_gate = jnp.sum(jnp.where(matches, gates_pair[:, :, None], 0.0), axis=1)
    targets = send_row.reshape(-1)
    valid_flat = send_valid.reshape(-1)
    row_ids = jnp.arange(row_count, dtype=jnp.int32)
    selector = ((targets[:, None] == row_ids[None, :]) & valid_flat[:, None]).astype(jnp.bfloat16)
    picked = jnp.dot(selector, normed, preferred_element_type=jnp.float32).astype(jnp.bfloat16)
    picked = picked.reshape(experts, most, model_width)
    returned = experts_layer(picked, w_gate, w_up, w_down, replica_count, tensor_count)
    summed = returned.reshape(experts * most, model_width).astype(jnp.float32)
    combine = jnp.where(
        (targets[None, :] == row_ids[:, None]) & valid_flat[None, :],
        send_gate.reshape(-1)[None, :],
        0.0,
    )
    moe = jnp.dot(combine, summed, precision=lax.Precision.HIGHEST)
    return (layer_state + moe).astype(jnp.bfloat16)


def solution(mesh):
    return jax.shard_map(
        on_device,
        mesh=mesh,
        in_specs=(
            P("dp", "tensor"),
            P("tensor", None),
            P(("dp", "tensor"), None),
            P(),
            P(),
            P(),
            P(),
            P(("dp", "tensor"), None, None),
            P(("dp", "tensor"), None, None),
            P(("dp", "tensor"), None, None),
        ),
        out_specs=P(("dp", "tensor"), None),
        check_vma=False,
    )
```

```python
import functools

import jax
import jax.numpy as jnp
from jax import lax
from jax.experimental import pallas as pl
from jax.experimental.pallas import tpu as pltpu
from jax.sharding import PartitionSpec as P

MESH = pl.DeviceIdType.MESH
LANES = 4


def ring_rank(position, count):
    upper = position // (count // 2)
    return (1 - upper) * 2 * position + upper * (2 * (count - 1 - position) + 1)


def project_kernel(count, x_ref, w_ref, out_ref, held, term, send_sem, recv_sem):
    dp = lax.axis_index("dp")
    rank = lax.axis_index("tensor")
    odd = rank % 2
    half = rank // 2
    here = (1 - odd) * half + odd * (count - 1 - half)
    right = ring_rank((here + 1) % count, count)
    left = ring_rank((here + count - 1) % count, count)
    rows = out_ref.shape[0]
    width = out_ref.shape[1] // LANES

    def own_term(lane, block):
        start = pl.multiple_of(ring_rank(block, count) * rows, rows)
        return jnp.dot(
            x_ref[pl.ds(start, rows), :],
            w_ref[:, lane * width : (lane + 1) * width],
            preferred_element_type=jnp.float32,
        )

    def block_of(lane, slot):
        if lane < LANES // 2:
            return (here + 2 * count - 1 - slot) % count
        return (here + 1 + slot) % count

    def copy(lane, slot):
        return pltpu.make_async_remote_copy(
            src_ref=held.at[lane, slot],
            dst_ref=held.at[lane, slot + 1],
            send_sem=send_sem.at[lane, slot],
            recv_sem=recv_sem.at[lane, slot + 1],
            device_id=(dp, right if lane < LANES // 2 else left),
            device_id_type=MESH,
        )

    def arrival(lane, slot):
        return pltpu.make_async_remote_copy(
            src_ref=held.at[lane, slot],
            dst_ref=held.at[lane, slot],
            send_sem=send_sem.at[lane, slot],
            recv_sem=recv_sem.at[lane, slot],
            device_id=(dp, right if lane < LANES // 2 else left),
            device_id_type=MESH,
        )

    order = [lane for k in range(LANES // 2) for lane in (k, LANES // 2 + k)]
    barrier = pltpu.get_barrier_semaphore()
    for neighbour in (left, right):
        pl.semaphore_signal(barrier, inc=1, device_id=(dp, neighbour), device_id_type=MESH)
    for n, lane in enumerate(order):
        held[lane, 0] = own_term(lane, block_of(lane, 0)).astype(held.dtype)
        if n == 0:
            pl.semaphore_wait(barrier, 2)
        copy(lane, 0).start()

    def step(slot, carry):
        for lane in order:
            term[lane] = own_term(lane, block_of(lane, slot))
        for lane in order:
            arrival(lane, slot).wait_recv()
            held[lane, slot] = (held[lane, slot].astype(jnp.float32) + term[lane]).astype(held.dtype)
            copy(lane, slot).start()
        return carry

    lax.fori_loop(1, count - 1, step, 0)
    last = count - 1
    for lane in order:
        term[lane] = own_term(lane, block_of(lane, last))
    for lane in order:
        arrival(lane, last).wait_recv()
        out_ref[:, lane * width : (lane + 1) * width] = (
            held[lane, last].astype(jnp.float32) + term[lane]
        )

    def drain(slot, carry):
        for lane in order:
            copy(lane, slot).wait_send()
        return carry

    lax.fori_loop(0, count - 1, drain, 0)


def project(x, w, count):
    rows = x.shape[0] // count
    columns = w.shape[1]
    width = columns // LANES
    return pl.pallas_call(
        functools.partial(project_kernel, count),
        out_shape=jax.ShapeDtypeStruct((rows, columns), jnp.float32),
        in_specs=[pl.BlockSpec(memory_space=pltpu.VMEM)] * 2,
        out_specs=pl.BlockSpec(memory_space=pltpu.VMEM),
        scratch_shapes=[
            pltpu.VMEM((LANES, count, rows, width), jnp.bfloat16),
            pltpu.VMEM((LANES, rows, width), jnp.float32),
            pltpu.SemaphoreType.DMA((LANES, count)),
            pltpu.SemaphoreType.DMA((LANES, count)),
        ],
        compiler_params=pltpu.CompilerParams(
            collective_id=0, has_side_effects=True, vmem_limit_bytes=48 * 1024 * 1024
        ),
    )(x, w)


class Place:
    def __init__(self, replicas, count):
        self.dp = lax.axis_index("dp")
        rank = lax.axis_index("tensor")
        self.odd = rank % 2
        self.replicas = replicas
        self.per_row = count // 2
        self.pairs = replicas * self.per_row
        self.pair = self.dp * self.per_row + rank // 2
        self.partner = (self.dp, rank + 1 - 2 * self.odd)

    def device(self, pair):
        return (pair // self.per_row, 2 * (pair % self.per_row) + self.odd)

    def shifted(self, k, sign):
        along, over = k // self.replicas, k % self.replicas
        row = (self.dp + self.replicas + sign * over) % self.replicas
        column = (self.pair % self.per_row + self.per_row + sign * along) % self.per_row
        return row * self.per_row + column

    def greet(self):
        barrier = pltpu.get_barrier_semaphore()

        def signal(k, carry):
            target = self.device((self.pair + k) % self.pairs)
            pl.semaphore_signal(barrier, inc=1, device_id=target, device_id_type=MESH)
            return carry

        lax.fori_loop(1, self.pairs, signal, 0)
        pl.semaphore_signal(barrier, inc=1, device_id=self.partner, device_id_type=MESH)
        pl.semaphore_wait(barrier, self.pairs)


def loop(start, stop, body):
    def step(k, carry):
        body(k)
        return carry

    lax.fori_loop(start, stop, step, 0)


PIECES = 4


def experts_kernel(
    replicas,
    count,
    group,
    x_ref,
    gate_hbm,
    up_hbm,
    down_hbm,
    out_ref,
    gate_w,
    up_w,
    down_w,
    received,
    result,
    part,
    weight_sem,
    send_sem,
    pass_sem,
    recv_sem,
    cross_sem,
    part_sem,
    home_sem,
    done_sem,
    keep_sem,
):
    at = Place(replicas, count)
    most, width = x_ref.shape[1:]
    rows = group * 2 * most
    groups = at.pairs // group

    def source(k):
        return at.shifted(k, -1)

    def outward(k):
        target = at.shifted(k, 1)
        return pltpu.make_async_remote_copy(
            src_ref=x_ref.at[target],
            dst_ref=received.at[k, at.odd],
            send_sem=send_sem.at[k],
            recv_sem=recv_sem.at[k, at.odd],
            device_id=at.device(target),
            device_id_type=MESH,
        )

    def sideways(k, side):
        return pltpu.make_async_remote_copy(
            src_ref=received.at[k, side],
            dst_ref=received.at[k, side],
            send_sem=pass_sem.at[k],
            recv_sem=recv_sem.at[k, side],
            device_id=at.partner,
            device_id_type=MESH,
        )

    def across(k):
        return pltpu.make_async_remote_copy(
            src_ref=result.at[k, 1 - at.odd],
            dst_ref=part.at[k],
            send_sem=cross_sem.at[k],
            recv_sem=part_sem.at[k],
            device_id=at.partner,
            device_id_type=MESH,
        )

    def home(k):
        return pltpu.make_async_remote_copy(
            src_ref=part.at[k],
            dst_ref=out_ref.at[at.pair],
            send_sem=home_sem.at[k],
            recv_sem=done_sem.at[at.pair],
            device_id=at.device(source(k)),
            device_id_type=MESH,
        )

    def forward(k):
        sideways(k, at.odd).wait_recv()
        sideways(k, at.odd).start()

    def add(k):
        across(k).wait_recv()
        part[k] = (
            part[k].astype(jnp.float32) + result[k, at.odd].astype(jnp.float32)
        ).astype(part.dtype)

    def add_and_send(k):
        add(k)
        home(k).start()

    loads = [
        pltpu.make_async_copy(hbm.at[0], vmem, weight_sem.at[n])
        for n, (hbm, vmem) in enumerate(((gate_hbm, gate_w), (up_hbm, up_w), (down_hbm, down_w)))
    ]
    for load in loads:
        load.start()
    own = pltpu.make_async_remote_copy(
        src_ref=x_ref.at[at.pair],
        dst_ref=received.at[0, at.odd],
        send_sem=pass_sem.at[0],
        recv_sem=recv_sem.at[0, at.odd],
        device_id=at.partner,
        device_id_type=MESH,
    )
    at.greet()
    loop(1, at.pairs, lambda k: outward(k).start())
    own.start()
    received[0, at.odd] = x_ref[at.pair]
    loop(1, group, forward)
    for load in loads:
        load.wait()
    contract = (((1,), (1,)), ((), ()))

    def step(g):
        first = g * group

        def forward_piece(piece):
            @pl.when(g + 1 < groups)
            def _():
                start = first + group
                cut = [start + n * group // PIECES for n in (piece, piece + 1)]
                loop(cut[0], cut[1], forward)

        loop(first, first + group, lambda k: sideways(k, 1 - at.odd).wait_recv())
        x = received[pl.ds(first, group)].reshape(rows, width)
        gate_part = lax.dot_general(x, gate_w[...], contract, preferred_element_type=jnp.float32)
        forward_piece(0)
        up_part = lax.dot_general(x, up_w[...], contract, preferred_element_type=jnp.float32)
        hidden = (gate_part / (1.0 + jnp.exp(-gate_part)) * up_part).astype(result.dtype)

        @pl.when(g > 0)
        def _():
            loop(jnp.maximum(first - group, 1), first, add_and_send)

        forward_piece(1)
        for piece in range(2):
            columns = slice(piece * (width // 2), (piece + 1) * (width // 2))
            y = jnp.dot(hidden, down_w[:, columns], preferred_element_type=jnp.float32)
            result[pl.ds(first, group), :, :, columns] = y.astype(result.dtype).reshape(
                group, 2, most, width // 2
            )
        loop(first, first + group, lambda k: across(k).start())
        forward_piece(2)
        forward_piece(3)

    loop(0, groups, step)
    loop(at.pairs - group, at.pairs, add_and_send)
    add(0)
    keep = pltpu.make_async_copy(part.at[0], out_ref.at[at.pair], keep_sem.at[0])
    keep.start()

    def settle(k):
        pair = source(k)
        pltpu.make_async_remote_copy(
            src_ref=part.at[k],
            dst_ref=out_ref.at[pair],
            send_sem=home_sem.at[k],
            recv_sem=done_sem.at[pair],
            device_id=at.partner,
            device_id_type=MESH,
        ).wait_recv()

    loop(1, at.pairs, settle)
    keep.wait()
    own.wait_send()
    across(0).wait_send()

    def drain(k):
        outward(k).wait_send()
        sideways(k, at.odd).wait_send()
        across(k).wait_send()
        home(k).wait_send()

    loop(1, at.pairs, drain)


def experts_layer(x, w_gate, w_up, w_down, replicas, count):
    pairs, most, width = x.shape
    group = min(pairs // 2, max(PIECES, 64 // most))
    hidden_units = w_gate.shape[1]
    weight = pltpu.VMEM((hidden_units, width), w_gate.dtype)
    return pl.pallas_call(
        functools.partial(experts_kernel, replicas, count, group),
        out_shape=jax.ShapeDtypeStruct(x.shape, x.dtype),
        in_specs=[pl.BlockSpec(memory_space=pltpu.VMEM)] + [pl.BlockSpec(memory_space=pl.ANY)] * 3,
        out_specs=pl.BlockSpec(memory_space=pl.ANY),
        scratch_shapes=[
            weight,
            weight,
            weight,
            pltpu.VMEM((pairs, 2, most, width), x.dtype),
            pltpu.VMEM((pairs, 2, most, width), x.dtype),
            pltpu.VMEM((pairs, most, width), x.dtype),
            pltpu.SemaphoreType.DMA((3,)),
            pltpu.SemaphoreType.DMA((pairs,)),
            pltpu.SemaphoreType.DMA((pairs,)),
            pltpu.SemaphoreType.DMA((pairs, 2)),
            pltpu.SemaphoreType.DMA((pairs,)),
            pltpu.SemaphoreType.DMA((pairs,)),
            pltpu.SemaphoreType.DMA((pairs,)),
            pltpu.SemaphoreType.DMA((pairs,)),
            pltpu.SemaphoreType.DMA((1,)),
        ],
        compiler_params=pltpu.CompilerParams(
            collective_id=1, has_side_effects=True, vmem_limit_bytes=56 * 1024 * 1024
        ),
    )(x, w_gate, w_up, w_down)


def on_device(
    head_outputs, out_weight, residual, norm_gain, chosen, gates, place, w_gate, w_up, w_down
):
    tensor_count = lax.axis_size("tensor")
    replica_count = lax.axis_size("dp")
    owners = replica_count * tensor_count
    my_index = lax.axis_index("dp") * tensor_count + lax.axis_index("tensor")
    row_count = residual.shape[0]
    model_width = residual.shape[1]
    projected = project(head_outputs, out_weight, tensor_count)
    layer_state = residual.astype(jnp.float32) + projected
    scale = lax.rsqrt(jnp.mean(layer_state * layer_state, axis=1, keepdims=True) + 1.0)
    normed = (layer_state * scale * norm_gain[None, :]).astype(jnp.bfloat16)
    experts = place.shape[0]
    capacity = chosen.shape[1]
    most = 2 * capacity // owners
    pair_map = (place[None, :] == jnp.arange(experts, dtype=jnp.int32)[:, None]).astype(jnp.float32)
    chosen_pair = jnp.dot(
        pair_map, chosen.astype(jnp.float32), precision=lax.Precision.HIGHEST
    ).astype(jnp.int32)
    gates_pair = jnp.dot(pair_map, gates, precision=lax.Precision.HIGHEST)
    local_row = chosen_pair - my_index * row_count
    is_mine = (local_row >= 0) & (local_row < row_count)
    mine_float = is_mine.astype(jnp.float32)
    capacity_ids = jnp.arange(capacity, dtype=jnp.int32)
    earlier = (capacity_ids[:, None] < capacity_ids[None, :]).astype(jnp.float32)
    slot_rank = jnp.dot(mine_float, earlier, precision=lax.Precision.HIGHEST).astype(jnp.int32)
    matches = is_mine[:, :, None] & (
        slot_rank[:, :, None] == jnp.arange(most, dtype=jnp.int32)[None, None, :]
    )
    match_count = matches.astype(jnp.int32)
    send_row = jnp.sum(match_count * local_row[:, :, None], axis=1)
    send_valid = jnp.sum(match_count, axis=1) > 0
    send_gate = jnp.sum(jnp.where(matches, gates_pair[:, :, None], 0.0), axis=1)
    targets = send_row.reshape(-1)
    valid_flat = send_valid.reshape(-1)
    row_ids = jnp.arange(row_count, dtype=jnp.int32)
    selector = ((targets[:, None] == row_ids[None, :]) & valid_flat[:, None]).astype(jnp.bfloat16)
    picked = jnp.dot(selector, normed, preferred_element_type=jnp.float32).astype(jnp.bfloat16)
    picked = picked.reshape(experts, most, model_width)
    returned = experts_layer(picked, w_gate, w_up, w_down, replica_count, tensor_count)
    summed = returned.reshape(experts * most, model_width).astype(jnp.float32)
    combine = jnp.where(
        (targets[None, :] == row_ids[:, None]) & valid_flat[None, :],
        send_gate.reshape(-1)[None, :],
        0.0,
    )
    moe = jnp.dot(combine, summed, precision=lax.Precision.HIGHEST)
    return (layer_state + moe).astype(jnp.bfloat16)


def solution(mesh):
    return jax.shard_map(
        on_device,
        mesh=mesh,
        in_specs=(
            P("dp", "tensor"),
            P("tensor", None),
            P(("dp", "tensor"), None),
            P(),
            P(),
            P(),
            P(),
            P(("dp", "tensor"), None, None),
            P(("dp", "tensor"), None, None),
            P(("dp", "tensor"), None, None),
        ),
        out_specs=P(("dp", "tensor"), None),
        check_vma=False,
    )
```
